32 devices in a mesh: seq: 8 (over z, y), head: 4 (over x, core).
Axes of the slice: x: 2, y: 2, z: 4, core: 2. Of those that a mesh axis runs over, the one named last changes fastest.
Arguments:
- queries: bfloat16 [1024, 24576], P('seq', 'head'), may hold values from -325 to 325
- latents: bfloat16 [1024, 576], P('seq'), may hold values from -5 to 5
- doc_ids: int32 [1024], P('seq'), may hold values from 0 to 3, never falling along the last dimension, each value on 1 to 512 neighbouring positions
- key_weight: bfloat16 [512, 16384], P(None, 'head'), may hold values from -0.25 to 0.25
- value_weight: bfloat16 [512, 16384], P(None, 'head'), may hold values from -0.25 to 0.25
- out_grad: bfloat16 [1024, 16384], P('seq', 'head'), may hold values from -6 to 6
Outputs:
- attended: bfloat16 [1024, 16384], P('seq', 'head')
- latent_grad: float32 [1024, 576], P('seq')
- key_weight_grad: float32 [512, 16384], P('seq', 'head')
- value_weight_grad: float32 [512, 16384], P('seq', 'head')
The draws below stay inside these ranges and needn't reach their ends.
Inputs may be any that keep to these rules, and one draw needn't show every extreme that they name: `doc_ids`: ids never fall along the sequence; every document holds 1 to 512 tokens, and one holds exactly that many.
All inputs are finite; a program needn't handle non-finite values.
Results may differ from the reference program's by a relative error of at most 0.028.
Values may be sent and summed in bfloat16 or wider, within the bound.
A program may use at most 128 MiB of HBM per device.

```python
import math
import jax
import jax.numpy as jnp
import numpy as np
from jax import lax

HEADS = 128
NOPE = 128
ROPE = 64
VDIM = 128
LATENT = 512
TOK_DEV = 128
REACH = 4
TOKENS = 1024
DOCS = 4


def base_latents(key):
    normal_rows = jax.random.normal(jax.random.fold_in(key, 7), (TOKENS, LATENT + ROPE), jnp.float32)
    return jnp.clip(normal_rows, -5.0, 5.0)


def draw_latents(key, part):
    drawn = base_latents(key)
    return drawn.astype(jnp.bfloat16)


def draw_queries(key, part):
    width = NOPE + ROPE
    drawn = jax.random.normal(jax.random.fold_in(key, 3), (TOKENS, HEADS, width), jnp.float32)
    drawn = jnp.clip(drawn, -5.0, 5.0)
    return drawn.reshape(TOKENS, HEADS * width).astype(jnp.bfloat16)


def shard_levels(stream_key, dims, shards, low, high):
    level = 1.0
    for dim, parts in shards:
        steps = jax.random.uniform(jax.random.fold_in(jax.random.fold_in(stream_key, 6), dim), (parts,), jnp.float32, low / len(shards), high / len(shards))
        level = level * jnp.repeat(jnp.exp(steps), dims[dim] // parts).reshape((-1,) + (1,) * (len(dims) - 1 - dim))
    return level


def split_up(count, total, limit, lean):
    weights = [(1 << 20) // math.isqrt(standing ** lean) + 1 for standing in range(2, count + 1)]
    rest, given = total - limit - (count - 1), [1] * (count - 1)
    while rest > 0:
        movable = [i for i in range(count - 1) if given[i] < limit]
        pool, budget = sum([weights[i] for i in movable]), rest
        for i in movable:
            more = min(limit - given[i], max(1, budget * weights[i] // pool), rest)
            given[i] = given[i] + more
            rest = rest - more
    return np.array([limit] + given)


def ragged_sizes(own_key, number_of, total, reach, lean):
    if number_of == 2:
        one = jax.random.randint(own_key, (), max(1, total - reach), min(reach, total - 1) + 1)
        return jnp.stack([one, total - one])
    sizes = jnp.asarray(split_up(number_of, total, reach, lean), jnp.int32)
    pairs = (number_of - 1) // 2
    giver, taker = sizes[1:1 + 2 * pairs:2], sizes[2:2 + 2 * pairs:2]
    room = jnp.minimum(giver - 1, reach - taker)
    passed = jax.random.randint(jax.random.fold_in(own_key, 1), (pairs,), 0, 1 << 20) % (room + 1)
    sizes = sizes.at[1:1 + 2 * pairs:2].set(giver - passed).at[2:2 + 2 * pairs:2].set(taker + passed)
    return sizes[jax.random.permutation(jax.random.fold_in(own_key, 2), number_of)]


def normal_values(own_key, extent, deviation, bound, split=(), held_as=jnp.bfloat16):
    factor_of = shard_levels(own_key, extent, split, -0.22, 0.18) if split else 1.0
    values = jax.random.normal(own_key, extent, jnp.float32) * deviation * factor_of
    return jnp.minimum(jnp.maximum(values, -bound), bound).astype(held_as)


def setup_inputs(seed: int = 0) -> dict:
    seeds = jax.random.split(jax.random.key(seed), 7)
    queries = draw_queries(jax.random.fold_in(seeds[6], 71), 0)
    latents = draw_latents(jax.random.fold_in(seeds[6], 71), 0)
    doc_ids = jnp.searchsorted(jnp.cumsum(ragged_sizes(seeds[2], DOCS, TOKENS, REACH * TOK_DEV, 1)), jnp.arange(TOKENS), side="right").astype(jnp.int32)
    key_weight = normal_values(seeds[3], (LATENT, HEADS * NOPE), LATENT ** -0.5, 0.25, ((1, 4),))
    value_weight = normal_values(seeds[4], (LATENT, HEADS * VDIM), LATENT ** -0.5, 0.25, ((1, 4),))
    out_grad = normal_values(seeds[5], (TOKENS, HEADS * VDIM), 1.0, 6.0, ((0, 8), (1, 4)))
    return {"queries": queries, "latents": latents, "doc_ids": doc_ids, "key_weight": key_weight, "value_weight": value_weight, "out_grad": out_grad}


def reference(queries, latents, doc_ids, key_weight, value_weight, out_grad):
    query_width = NOPE + ROPE
    score_scale = 1.0 / (query_width ** 0.5)
    block_count = TOKENS // TOK_DEV
    key_rows = (REACH + 1) * TOK_DEV
    lead_rows = REACH * TOK_DEV
    latent_part = latents[:, :LATENT]
    k_nope = jnp.dot(latent_part, key_weight, preferred_element_type=jnp.float32).astype(jnp.bfloat16)
    values_up = jnp.dot(latent_part, value_weight, preferred_element_type=jnp.float32).astype(jnp.bfloat16)
    nope_pad = jnp.concatenate([jnp.zeros((lead_rows, HEADS * NOPE), jnp.bfloat16), k_nope], axis=0)
    value_pad = jnp.concatenate([jnp.zeros((lead_rows, HEADS * VDIM), jnp.bfloat16), values_up], axis=0)
    rope_pad = jnp.concatenate([jnp.zeros((lead_rows, ROPE), jnp.bfloat16), latents[:, LATENT:]], axis=0)
    latent_pad = jnp.concatenate([jnp.zeros((lead_rows, LATENT), jnp.bfloat16), latent_part], axis=0)
    ids_pad = jnp.concatenate([jnp.full((lead_rows,), -1, jnp.int32), doc_ids.astype(jnp.int32)], axis=0)
    pos_pad = jnp.arange(TOKENS + lead_rows, dtype=jnp.int32) - lead_rows

    def block_step(totals, block_index):
        first_row = (block_index * TOK_DEV).astype(jnp.int32)
        query_heads = lax.dynamic_slice_in_dim(queries, first_row, TOK_DEV, 0).reshape(TOK_DEV, HEADS, query_width).astype(jnp.float32)
        grad_heads = lax.dynamic_slice_in_dim(out_grad, first_row, TOK_DEV, 0).reshape(TOK_DEV, HEADS, VDIM).astype(jnp.float32)
        query_ids = lax.dynamic_slice_in_dim(doc_ids.astype(jnp.int32), first_row, TOK_DEV, 0)
        query_pos = first_row + jnp.arange(TOK_DEV, dtype=jnp.int32)
        key_heads = lax.dynamic_slice_in_dim(nope_pad, first_row, key_rows, 0)
        value_heads = lax.dynamic_slice_in_dim(value_pad, first_row, key_rows, 0)
        key_rope = lax.dynamic_slice_in_dim(rope_pad, first_row, key_rows, 0).astype(jnp.float32)
        latent_rows = lax.dynamic_slice_in_dim(latent_pad, first_row, key_rows, 0)
        key_ids = lax.dynamic_slice_in_dim(ids_pad, first_row, key_rows, 0)
        key_pos = lax.dynamic_slice_in_dim(pos_pad, first_row, key_rows, 0)
        key_f = key_heads.reshape(key_rows, HEADS, NOPE).astype(jnp.float32)
        value_f = value_heads.reshape(key_rows, HEADS, VDIM).astype(jnp.float32)
        scores = jnp.einsum("phd,thd->hpt", query_heads[:, :, :NOPE], key_f, precision=lax.Precision.HIGHEST)
        scores = scores + jnp.einsum("phr,tr->hpt", query_heads[:, :, NOPE:], key_rope, precision=lax.Precision.HIGHEST)
        scores = scores * score_scale
        visible = (key_pos[None, :] <= query_pos[:, None]) & (key_ids[None, :] == query_ids[:, None])
        scores = jnp.where(visible[None], scores, -jnp.inf)
        row_top = jnp.max(scores, axis=-1, keepdims=True)
        row_lse = row_top + jnp.log(jnp.sum(jnp.exp(scores - row_top), axis=-1, keepdims=True))
        weight_f = jnp.exp(scores - row_lse)
        weight_b = weight_f.astype(jnp.bfloat16)
        output = jnp.einsum("hpt,thd->phd", weight_b.astype(jnp.float32), value_f, precision=lax.Precision.HIGHEST).astype(jnp.bfloat16)
        d_weight = jnp.einsum("phd,thd->hpt", grad_heads, value_f, precision=lax.Precision.HIGHEST)
        row_delta = jnp.sum(grad_heads * output.astype(jnp.float32), axis=-1)
        d_score = (weight_f * (d_weight - jnp.transpose(row_delta)[:, :, None]) * score_scale).astype(jnp.bfloat16)
        d_key = jnp.einsum("hpt,phd->thd", d_score.astype(jnp.float32), query_heads, precision=lax.Precision.HIGHEST).astype(jnp.bfloat16)
        d_value = jnp.einsum("hpt,phd->thd", weight_b.astype(jnp.float32), grad_heads, precision=lax.Precision.HIGHEST).astype(jnp.bfloat16)
        key_nope_grad = d_key[:, :, :NOPE].reshape(key_rows, HEADS * NOPE)
        value_grad = d_value.reshape(key_rows, HEADS * VDIM)
        latent_term = jnp.dot(key_nope_grad, jnp.transpose(key_weight), preferred_element_type=jnp.float32)
        latent_term = latent_term + jnp.dot(value_grad, jnp.transpose(value_weight), preferred_element_type=jnp.float32)
        rope_term = jnp.sum(d_key[:, :, NOPE:].astype(jnp.float32), axis=1)
        partial_grad = jnp.concatenate([latent_term, rope_term], axis=1)
        key_total = totals[0] + jnp.dot(jnp.transpose(latent_rows), key_nope_grad, preferred_element_type=jnp.float32)
        value_total = totals[1] + jnp.dot(jnp.transpose(latent_rows), value_grad, preferred_element_type=jnp.float32)
        return (key_total, value_total), (output.reshape(TOK_DEV, HEADS * VDIM), partial_grad)

    start_totals = (jnp.zeros((LATENT, HEADS * NOPE), jnp.float32), jnp.zeros((LATENT, HEADS * VDIM), jnp.float32))
    totals, emitted = lax.scan(block_step, start_totals, jnp.arange(block_count, dtype=jnp.int32))
    attended = emitted[0].reshape(TOKENS, HEADS * VDIM)
    pieces = emitted[1].reshape(block_count, REACH + 1, TOK_DEV, LATENT + ROPE)
    summed = jnp.zeros((block_count + REACH, TOK_DEV, LATENT + ROPE), jnp.float32)
    for offset in range(REACH + 1):
        summed = summed + jnp.pad(pieces[:, offset], ((offset, REACH - offset), (0, 0), (0, 0)))
    latent_grad = summed[REACH:].reshape(TOKENS, LATENT + ROPE)
    return attended, latent_grad, totals[0], totals[1]
```

```python
import functools
import math

import jax
import jax.numpy as jnp
from jax import lax
from jax.experimental import pallas as pl
from jax.experimental.pallas import tpu as pltpu
from jax.sharding import PartitionSpec as P

NOPE = 128
ROPE = 64
VDIM = 128
LATENT = 512
REACH = 4
PAIR = 2
Y_LAG = 2
Z_LAG = 2
MESH = pl.DeviceIdType.MESH
F32 = jnp.float32
BF16 = jnp.bfloat16


def dot(a, b, ca, cb):
    return lax.dot_general(a, b, (((ca,), (cb,)), ((), ())), preferred_element_type=F32)


def kernel(
    n, hn, steps, grid_steps,
    latx_ref, qid_ref, q_ref, g_ref, kw_ref, vw_ref,
    att_ref, lg_ref, kwg_ref, vwg_ref,
    lat_all, lat_t, bias, lgacc, part, ry, rzp, rzm, ls, lr, hb,
    lat_ss, lat_rs, y_ss, y_rs, z_ss, zp_rs, zm_rs, l_ss, l_rs, h_ss, h_rs,
):
    j = pl.program_id(0)
    s = lax.axis_index("seq")
    h = lax.axis_index("head")
    line = n // 2
    z, y = s // 2, s % 2
    tok = latx_ref.shape[0]
    keys = (REACH + 1) * tok
    scale = 1.0 / math.sqrt(NOPE + ROPE)

    def lat_copy(d):
        return pltpu.make_async_remote_copy(
            src_ref=latx_ref,
            dst_ref=lat_all.at[pl.ds((REACH - d) * tok, tok)],
            send_sem=lat_ss.at[d - 1], recv_sem=lat_rs.at[d - 1],
            device_id=(s + d, h), device_id_type=MESH,
        )

    def y_copy(i):
        return pltpu.make_async_remote_copy(
            src_ref=part.at[i, 1 - y], dst_ref=ry.at[i],
            send_sem=y_ss.at[i], recv_sem=y_rs.at[i],
            device_id=(s + 1 - 2 * y, h), device_id_type=MESH,
        )

    def z_copy(i, d, up):
        return pltpu.make_async_remote_copy(
            src_ref=part.at[i, y, d], dst_ref=(rzp if up else rzm).at[i, d],
            send_sem=z_ss.at[i, d], recv_sem=(zp_rs if up else zm_rs).at[i, d],
            device_id=(s + 2 if up else s - 2, h), device_id_type=MESH,
        )

    def l_copy(d):
        return pltpu.make_async_remote_copy(
            src_ref=ls.at[d - 1], dst_ref=lr.at[d - 1],
            send_sem=l_ss.at[d - 1], recv_sem=l_rs.at[d - 1],
            device_id=(s - d, h), device_id_type=MESH,
        )

    def h_copy(k, slot):
        return pltpu.make_async_remote_copy(
            src_ref=hb.at[slot], dst_ref=hb.at[slot],
            send_sem=h_ss.at[k - 1], recv_sem=h_rs.at[slot],
            device_id=(s, (h + k) % hn), device_id_type=MESH,
        )

    @pl.when(j == 0)
    def _():
        barrier = pltpu.get_barrier_semaphore()
        for d in range(1, REACH + 1):
            @pl.when(s + d < n)
            def _():
                pl.semaphore_signal(barrier, inc=1, device_id=(s + d, h), device_id_type=MESH)

            @pl.when(s - d >= 0)
            def _():
                pl.semaphore_signal(barrier, inc=1, device_id=(s - d, h), device_id_type=MESH)
        for k in range(1, hn):
            pl.semaphore_signal(barrier, inc=1, device_id=(s, (h + k) % hn), device_id_type=MESH)
        pl.semaphore_wait(barrier, jnp.minimum(s, REACH) + jnp.minimum(n - 1 - s, REACH) + hn - 1)
        for d in range(1, REACH + 1):
            @pl.when(s + d < n)
            def _():
                lat_copy(d).start()
        lat_all[REACH * tok:, :] = latx_ref[...]
        lgacc[...] = jnp.zeros_like(lgacc)
        for d in range(1, REACH + 1):
            @pl.when(s - d >= 0)
            def _():
                lat_copy(d).wait_recv()

            @pl.when(s - d < 0)
            def _():
                lat_all[(REACH - d) * tok:(REACH - d + 1) * tok, :] = jnp.zeros((tok, latx_ref.shape[1]), BF16)
        for d in range(1, REACH + 1):
            @pl.when(s + d < n)
            def _():
                lat_copy(d).wait_send()
        lat_t[...] = jnp.transpose(lat_all[:, :LATENT])
        key_row = lax.broadcasted_iota(jnp.int32, (keys, tok), 0)
        query_row = lax.broadcasted_iota(jnp.int32, (keys, tok), 1) + REACH * tok
        key_id = lat_all[:, LATENT + ROPE:LATENT + ROPE + 1].astype(F32)
        visible = (
            (key_row <= query_row)
            & (key_row >= (REACH - s) * tok)
            & (key_id == qid_ref[...])
        )
        bias[...] = jnp.where(visible, 0.0, -jnp.inf)

    @pl.when(j < steps)
    def _():
        lat = lat_all[:, :LATENT]
        rope = lat_all[:, LATENT:LATENT + ROPE]
        kw, vw = kw_ref[...], vw_ref[...]
        k2 = dot(lat, kw, 1, 0).astype(BF16)
        v2 = dot(lat, vw, 1, 0).astype(BF16)
        dks, dvs, rope_sum = [], [], None
        for a in range(PAIR):
            q = q_ref[:, a * (NOPE + ROPE):(a + 1) * (NOPE + ROPE)]
            g = g_ref[:, a * VDIM:(a + 1) * VDIM]
            v = v2[:, a * VDIM:(a + 1) * VDIM]
            k = jnp.concatenate([k2[:, a * NOPE:(a + 1) * NOPE], rope], axis=1)
            sc = dot(k, q, 1, 1) * scale + bias[...]
            e = jnp.exp(sc - jnp.max(sc, axis=0, keepdims=True))
            p = e * (1.0 / jnp.sum(e, axis=0, keepdims=True))
            pb = p.astype(BF16)
            att_ref[:, a * VDIM:(a + 1) * VDIM] = dot(pb, v, 0, 0).astype(BF16)
            dp = dot(v, g, 1, 1)
            delta = jnp.sum(pb.astype(F32) * dp, axis=0, keepdims=True)
            ds = (p * (dp - delta) * scale).astype(BF16)
            dk = dot(ds, q, 1, 0).astype(BF16)
            dvs.append(dot(pb, g, 1, 0).astype(BF16))
            dks.append(dk[:, :NOPE])
            r = dk[:, NOPE:].astype(F32)
            rope_sum = r if rope_sum is None else rope_sum + r
        dk2 = jnp.concatenate(dks, axis=1)
        dv2 = jnp.concatenate(dvs, axis=1)
        lgacc[:, :LATENT] += dot(dk2, kw, 1, 1) + dot(dv2, vw, 1, 1)
        lgacc[:, LATENT:] += rope_sum
        lt = lat_t[...]
        rows = part.shape[3]
        for col, dd in ((0, dk2), (PAIR * NOPE, dv2)):
            wg = dot(lt, dd, 1, 0).astype(BF16).reshape(line, 2, rows, dd.shape[1])
            for yy in range(2):
                part[j, yy, :, :, col:col + dd.shape[1]] = wg[:, yy]
        y_copy(j).start()

    @pl.when(j == steps - 1)
    def _():
        for d in range(1, REACH + 1):
            ls[d - 1] = lgacc[(REACH - d) * tok:(REACH - d + 1) * tok, :].astype(BF16)
        for d in range(1, REACH + 1):
            @pl.when(s - d >= 0)
            def _():
                l_copy(d).start()

    @pl.when(j == steps + 1)
    def _():
        for d in range(1, REACH + 1):
            @pl.when(s + d < n)
            def _():
                l_copy(d).wait_recv()
                lgacc[REACH * tok:, :] += lr[d - 1].astype(F32)
        hb[h] = lgacc[REACH * tok:, :].astype(BF16)
        for k in range(1, hn):
            h_copy(k, h).start()

    @pl.when(j == steps + 3)
    def _():
        for k in range(1, hn):
            h_copy(k, (h + k) % hn).wait_recv()
        total = hb[0].astype(F32)
        for k in range(1, hn):
            total = total + hb[k].astype(F32)
        lg_ref[...] = total

    iy = j - Y_LAG

    @pl.when((iy >= 0) & (iy < steps))
    def _():
        y_copy(iy).wait_recv()
        part[iy, y] = (part[iy, y].astype(F32) + ry[iy].astype(F32)).astype(BF16)

    for up in (True, False):
        pos = z if up else line - 1 - z
        iz = j - Y_LAG - Z_LAG * pos
        buf = rzp if up else rzm

        @pl.when((iz >= 0) & (iz < steps))
        def _():
            for dist in range(1, line):
                d = z + dist if up else z - dist

                @pl.when((d < line) & (d >= 0))
                def _():
                    @pl.when(pos > 0)
                    def _():
                        z_copy(iz, d, up).wait_recv()
                        part[iz, y, d] = (part[iz, y, d].astype(F32) + buf[iz, d].astype(F32)).astype(BF16)
                    z_copy(iz, d, up).start()

    fin = j - Y_LAG - Z_LAG * (line - 1)

    @pl.when((fin >= 0) & (fin < steps))
    def _():
        half = PAIR * NOPE
        own = part[fin, y, z].astype(F32)
        kwg_ref[...] = own[:, :half]
        vwg_ref[...] = own[:, half:]
        for up in (True, False):
            buf = rzp if up else rzm

            @pl.when(z > 0 if up else z < line - 1)
            def _():
                z_copy(fin, z, up).wait_recv()
                got = buf[fin, z].astype(F32)
                kwg_ref[...] += got[:, :half]
                vwg_ref[...] += got[:, half:]

    @pl.when(j == grid_steps - 1)
    def _():
        for d in range(1, REACH + 1):
            @pl.when(s - d >= 0)
            def _():
                l_copy(d).wait_send()
        for k in range(1, hn):
            h_copy(k, h).wait_send()

        def drain(i, c):
            y_copy(i).wait_send()
            for d in range(line):
                @pl.when(d != z)
                def _():
                    z_copy(i, d, True).wait_send()
            return c

        lax.fori_loop(0, steps, drain, 0)


def per_device(n, hn, queries, latents, doc_ids, key_weight, value_weight, out_grad):
    tok = latents.shape[0]
    heads = key_weight.shape[1] // NOPE
    steps = heads // PAIR
    line = n // 2
    rows = LATENT // n
    lag = Y_LAG + Z_LAG * (line - 1)
    grid_steps = steps + max(lag, 4)
    keys = (REACH + 1) * tok
    width = LATENT + ROPE
    latx = jnp.concatenate(
        [latents, jnp.broadcast_to(doc_ids.astype(BF16)[:, None], (tok, 64))], axis=1
    )
    qid = doc_ids.astype(F32)[None, :]
    whole = pl.BlockSpec(memory_space=pltpu.VMEM)

    def at(lag_by):
        return lambda j: (0, jnp.clip(j - lag_by, 0, steps - 1))

    dma = pltpu.SemaphoreType.DMA
    att, lg, kwg, vwg = pl.pallas_call(
        functools.partial(kernel, n, hn, steps, grid_steps),
        grid=(grid_steps,),
        out_shape=(
            jax.ShapeDtypeStruct((tok, heads * VDIM), BF16),
            jax.ShapeDtypeStruct((tok, width), F32),
            jax.ShapeDtypeStruct((rows, heads * NOPE), F32),
            jax.ShapeDtypeStruct((rows, heads * VDIM), F32),
        ),
        in_specs=[
            whole,
            whole,
            pl.BlockSpec((tok, PAIR * (NOPE + ROPE)), at(0)),
            pl.BlockSpec((tok, PAIR * VDIM), at(0)),
            pl.BlockSpec((LATENT, PAIR * NOPE), at(0)),
            pl.BlockSpec((LATENT, PAIR * VDIM), at(0)),
        ],
        out_specs=(
            pl.BlockSpec((tok, PAIR * VDIM), at(0)),
            whole,
            pl.BlockSpec((rows, PAIR * NOPE), at(lag)),
            pl.BlockSpec((rows, PAIR * VDIM), at(lag)),
        ),
        scratch_shapes=[
            pltpu.VMEM((keys, latx.shape[1]), BF16),
            pltpu.VMEM((LATENT, keys), BF16),
            pltpu.VMEM((keys, tok), F32),
            pltpu.VMEM((keys, width), F32),
            pltpu.VMEM((steps, 2, line, rows, PAIR * (NOPE + VDIM)), BF16),
            pltpu.VMEM((steps, line, rows, PAIR * (NOPE + VDIM)), BF16),
            pltpu.VMEM((steps, line, rows, PAIR * (NOPE + VDIM)), BF16),
            pltpu.VMEM((steps, line, rows, PAIR * (NOPE + VDIM)), BF16),
            pltpu.VMEM((REACH, tok, width), BF16),
            pltpu.VMEM((REACH, tok, width), BF16),
            pltpu.VMEM((hn, tok, width), BF16),
            dma((REACH,)), dma((REACH,)),
            dma((steps,)), dma((steps,)),
            dma((steps, line)), dma((steps, line)), dma((steps, line)),
            dma((REACH,)), dma((REACH,)),
            dma((max(hn - 1, 1),)), dma((hn,)),
        ],
        compiler_params=pltpu.CompilerParams(
            collective_id=0,
            has_side_effects=True,
            dimension_semantics=("arbitrary",),
            vmem_limit_bytes=60 * 1024 * 1024,
        ),
    )(latx, qid, queries, out_grad, key_weight, value_weight)
    return att, lg, kwg, vwg


def solution(mesh):
    in_specs = (
        P("seq", "head"),
        P("seq", None),
        P("seq"),
        P(None, "head"),
        P(None, "head"),
        P("seq", "head"),
    )
    out_specs = (P("seq", "head"), P("seq", None), P("seq", "head"), P("seq", "head"))
    body = functools.partial(per_device, mesh.shape["seq"], mesh.shape["head"])
    return jax.shard_map(
        body, mesh=mesh, in_specs=in_specs, out_specs=out_specs, check_vma=False
    )
```

```python
import functools
import math

import jax
import jax.numpy as jnp
from jax import lax
from jax.experimental import pallas as pl
from jax.experimental.pallas import tpu as pltpu
from jax.sharding import PartitionSpec as P

NOPE = 128
ROPE = 64
VDIM = 128
LATENT = 512
REACH = 4
PAIR = 2
Y_LAG = 8
Z_LAG = 2
F_LAG = 3
MESH = pl.DeviceIdType.MESH
F32 = jnp.float32
BF16 = jnp.bfloat16


def dot(a, b, ca, cb):
    return lax.dot_general(a, b, (((ca,), (cb,)), ((), ())), preferred_element_type=F32)


def line_first(i, steps):
    return (i % 4 == 1) & (i < steps // 2)


def kernel(
    n, hn, steps, grid_steps, fin_lag,
    lat_ref, qid_ref, q_ref, g_ref, kw_ref, vw_ref,
    att_ref, lg_ref, kwg_ref, vwg_ref,
    latx, lat_all, lat_t, bias, lgacc, part, ry, rzp, rzm, ls, lr, hb,
    lat_ss, lat_rs, f_ss, f_rs, y_ss, y_rs, z_ss, zp_rs, zm_rs, l_ss, l_rs, h_ss, h_rs,
):
    j = pl.program_id(0)
    s = lax.axis_index("seq")
    h = lax.axis_index("head")
    line = n // 2
    z, y = s // 2, s % 2
    tok = lat_ref.shape[0]

    keys = (REACH + 1) * tok
    scale = 1.0 / math.sqrt(NOPE + ROPE)

    def lat_copy(d):
        return pltpu.make_async_remote_copy(
            src_ref=latx.at[h],
            dst_ref=lat_all.at[REACH - d, h],
            send_sem=lat_ss.at[d - 1], recv_sem=lat_rs.at[d - 1],
            device_id=(s + d, h), device_id_type=MESH,
        )

    def f_copy(d, k, slot):
        return pltpu.make_async_remote_copy(
            src_ref=lat_all.at[REACH - d, slot],
            dst_ref=lat_all.at[REACH - d, slot],
            send_sem=f_ss.at[k - 1, d - 1], recv_sem=f_rs.at[slot, d - 1],
            device_id=(s, (h + k) % hn), device_id_type=MESH,
        )

    def y_late_copy(i):
        return pltpu.make_async_remote_copy(
            src_ref=part.at[i, 1 - y, z], dst_ref=ry.at[i, 0],
            send_sem=y_ss.at[i], recv_sem=y_rs.at[i],
            device_id=(s + 1 - 2 * y, h), device_id_type=MESH,
        )

    def y_copy(i):
        return pltpu.make_async_remote_copy(
            src_ref=part.at[i, 1 - y], dst_ref=ry.at[i],
            send_sem=y_ss.at[i], recv_sem=y_rs.at[i],
            device_id=(s + 1 - 2 * y, h), device_id_type=MESH,
        )

    def z_copy(i, d, up, both):
        buf = rzp if up else rzm
        return pltpu.make_async_remote_copy(
            src_ref=part.at[i, :, d] if both else part.at[i, y, d],
            dst_ref=buf.at[i, :, d] if both else buf.at[i, y, d],
            send_sem=z_ss.at[i, d], recv_sem=(zp_rs if up else zm_rs).at[i, d],
            device_id=(s + 2 if up else s - 2, h), device_id_type=MESH,
        )

    def l_copy(d):
        return pltpu.make_async_remote_copy(
            src_ref=ls.at[d - 1], dst_ref=lr.at[d - 1],
            send_sem=l_ss.at[d - 1], recv_sem=l_rs.at[d - 1],
            device_id=(s - d, h), device_id_type=MESH,
        )

    def h_copy(k, slot):
        return pltpu.make_async_remote_copy(
            src_ref=hb.at[slot], dst_ref=hb.at[slot],
            send_sem=h_ss.at[k - 1], recv_sem=h_rs.at[slot],
            device_id=(s, (h + k) % hn), device_id_type=MESH,
        )

    @pl.when(j == 0)
    def _():
        ids = jnp.transpose(jnp.broadcast_to(qid_ref[...].astype(F32), (tok, tok)))
        lx = jnp.concatenate([lat_ref[...], ids[:, :latx.shape[2] - lat_ref.shape[1]].astype(BF16)], axis=1)
        latx[...] = lx.reshape(latx.shape)
        barrier = pltpu.get_barrier_semaphore()
        for d in range(1, REACH + 1):
            @pl.when(s + d < n)
            def _():
                pl.semaphore_signal(barrier, inc=1, device_id=(s + d, h), device_id_type=MESH)

            @pl.when(s - d >= 0)
            def _():
                pl.semaphore_signal(barrier, inc=1, device_id=(s - d, h), device_id_type=MESH)
        for k in range(1, hn):
            pl.semaphore_signal(barrier, inc=1, device_id=(s, (h + k) % hn), device_id_type=MESH)
        pl.semaphore_wait(barrier, jnp.minimum(s, REACH) + jnp.minimum(n - 1 - s, REACH) + hn - 1)
        for d in range(1, REACH + 1):
            @pl.when(s + d < n)
            def _():
                lat_copy(d).start()
        lat_all[REACH] = latx[...]
        lgacc[...] = jnp.zeros_like(lgacc)
        for d in range(1, REACH + 1):
            @pl.when(s - d >= 0)
            def _():
                lat_copy(d).wait_recv()
                for k in range(1, hn):
                    f_copy(d, k, h).start()

            @pl.when(s - d < 0)
            def _():
                lat_all[REACH - d] = jnp.zeros(lat_all.shape[1:], BF16)
        for d in range(1, REACH + 1):
            @pl.when(s - d >= 0)
            def _():
                for k in range(1, hn):
                    f_copy(d, k, (h + k) % hn).wait_recv()
        lat_t[...] = jnp.transpose(lat_all[...].reshape(keys, lat_all.shape[3])[:, :LATENT])
        key_row = lax.broadcasted_iota(jnp.int32, (keys, tok), 0)
        query_row = lax.broadcasted_iota(jnp.int32, (keys, tok), 1) + REACH * tok
        key_id = lat_all[...].reshape(keys, lat_all.shape[3])[:, LATENT + ROPE:LATENT + ROPE + 1].astype(F32)
        visible = (
            (key_row <= query_row)
            & (key_row >= (REACH - s) * tok)
            & (key_id == qid_ref[...].astype(F32))
        )
        bias[...] = jnp.where(visible, 0.0, -jnp.inf)

    @pl.when(j < steps)
    def _():
        lat_rows = lat_all[...].reshape(keys, lat_all.shape[3])
        lat = lat_rows[:, :LATENT]
        rope = lat_rows[:, LATENT:LATENT + ROPE]
        kw, vw = kw_ref[...], vw_ref[...]
        k2 = dot(lat, kw, 1, 0).astype(BF16)
        v2 = dot(lat, vw, 1, 0).astype(BF16)
        dks, dvs, rope_sum = [], [], None
        for a in range(PAIR):
            q = q_ref[:, a * (NOPE + ROPE):(a + 1) * (NOPE + ROPE)]
            g = g_ref[:, a * VDIM:(a + 1) * VDIM]
            v = v2[:, a * VDIM:(a + 1) * VDIM]
            k = jnp.concatenate([k2[:, a * NOPE:(a + 1) * NOPE], rope], axis=1)
            sc = dot(k, q, 1, 1) * scale + bias[...]
            e = jnp.exp(sc - jnp.max(sc, axis=0, keepdims=True))
            p = e * (1.0 / jnp.sum(e, axis=0, keepdims=True))
            pb = p.astype(BF16)
            att_ref[:, a * VDIM:(a + 1) * VDIM] = dot(pb, v, 0, 0).astype(BF16)
            dp = dot(v, g, 1, 1)
            delta = jnp.sum(pb.astype(F32) * dp, axis=0, keepdims=True)
            ds = (p * (dp - delta) * scale).astype(BF16)
            dk = dot(ds, q, 1, 0).astype(BF16)
            dvs.append(dot(pb, g, 1, 0).astype(BF16))
            dks.append(dk[:, :NOPE])
            r = dk[:, NOPE:].astype(F32)
            rope_sum = r if rope_sum is None else rope_sum + r
        dk2 = jnp.concatenate(dks, axis=1)
        dv2 = jnp.concatenate(dvs, axis=1)
        lgacc[:, :LATENT] += dot(dk2, kw, 1, 1) + dot(dv2, vw, 1, 1)
        lgacc[:, LATENT:] += rope_sum
        lt = lat_t[...]
        rows = part.shape[3]
        for col, dd in ((0, dk2), (PAIR * NOPE, dv2)):
            wg = dot(lt, dd, 1, 0).astype(BF16).reshape(line, 2, rows, dd.shape[1])
            for yy in range(2):
                part[j, yy, :, :, col:col + dd.shape[1]] = wg[:, yy]
        @pl.when(jnp.logical_not(line_first(j, steps)))
        def _():
            y_copy(j).start()

    @pl.when(j == steps - 1)
    def _():
        for d in range(1, REACH + 1):
            ls[d - 1] = lgacc[(REACH - d) * tok:(REACH - d + 1) * tok, :].astype(BF16)
        for d in range(1, REACH + 1):
            @pl.when(s - d >= 0)
            def _():
                l_copy(d).start()

    @pl.when(j == steps + 1)
    def _():
        for d in range(1, REACH + 1):
            @pl.when(s + d < n)
            def _():
                l_copy(d).wait_recv()
                lgacc[REACH * tok:, :] += lr[d - 1].astype(F32)
        hb[h] = lgacc[REACH * tok:, :].astype(BF16)
        for k in range(1, hn):
            h_copy(k, h).start()

    @pl.when(j == steps + 3)
    def _():
        for k in range(1, hn):
            h_copy(k, (h + k) % hn).wait_recv()
        total = hb[0].astype(F32)
        for k in range(1, hn):
            total = total + hb[k].astype(F32)
        lg_ref[...] = total

    iy = j - Y_LAG

    @pl.when((iy >= 0) & (iy < steps) & jnp.logical_not(line_first(iy, steps)))
    def _():
        y_copy(iy).wait_recv()
        part[iy, y] = (part[iy, y].astype(F32) + ry[iy].astype(F32)).astype(BF16)

    def hop(iz, pos, up, both):
        buf = rzp if up else rzm
        which = slice(None) if both else y
        for dist in range(1, line):
            d = z + dist if up else z - dist

            @pl.when((d < line) & (d >= 0))
            def _():
                @pl.when(pos > 0)
                def _():
                    z_copy(iz, d, up, both).wait_recv()
                    part[iz, which, d] = (part[iz, which, d].astype(F32) + buf[iz, which, d].astype(F32)).astype(BF16)
                z_copy(iz, d, up, both).start()

    for both in (True, False):
        for up in (True, False):
            pos = z if up else line - 1 - z
            iz = j - F_LAG * pos if both else j - Y_LAG - Z_LAG * pos

            @pl.when((iz >= 0) & (iz < steps) & (line_first(iz, steps) == both))
            def _():
                hop(iz, pos, up, both)

    il = j - F_LAG * (line - 1) - 1

    @pl.when((il >= 0) & (il < steps) & line_first(il, steps))
    def _():
        for up in (True, False):
            buf = rzp if up else rzm

            @pl.when(z > 0 if up else z < line - 1)
            def _():
                z_copy(il, z, up, True).wait_recv()
                part[il, :, z] = (part[il, :, z].astype(F32) + buf[il, :, z].astype(F32)).astype(BF16)
        y_late_copy(il).start()

    fin = j - fin_lag
    half = PAIR * NOPE

    @pl.when((fin >= 0) & (fin < steps))
    def _():
        own = part[fin, y, z].astype(F32)
        kwg_ref[...] = own[:, :half]
        vwg_ref[...] = own[:, half:]

        @pl.when(line_first(fin, steps))
        def _():
            y_late_copy(fin).wait_recv()
            got = ry[fin, 0].astype(F32)
            kwg_ref[...] += got[:, :half]
            vwg_ref[...] += got[:, half:]

        @pl.when(jnp.logical_not(line_first(fin, steps)))
        def _():
            for up in (True, False):
                buf = rzp if up else rzm

                @pl.when(z > 0 if up else z < line - 1)
                def _():
                    z_copy(fin, z, up, False).wait_recv()
                    got = buf[fin, y, z].astype(F32)
                    kwg_ref[...] += got[:, :half]
                    vwg_ref[...] += got[:, half:]

    @pl.when(j == grid_steps - 1)
    def _():
        for d in range(1, REACH + 1):
            @pl.when(s - d >= 0)
            def _():
                l_copy(d).wait_send()
        for k in range(1, hn):
            h_copy(k, h).wait_send()

        for d in range(1, REACH + 1):
            @pl.when(s + d < n)
            def _():
                lat_copy(d).wait_send()

            @pl.when(s - d >= 0)
            def _():
                for k in range(1, hn):
                    f_copy(d, k, h).wait_send()

        def drain(i, c):
            for both in (True, False):
                @pl.when(line_first(i, steps) == both)
                def _():
                    (y_late_copy if both else y_copy)(i).wait_send()
                    for d in range(line):
                        @pl.when(d != z)
                        def _():
                            z_copy(i, d, True, both).wait_send()
            return c

        lax.fori_loop(0, steps, drain, 0)


def per_device(n, hn, queries, latents, doc_ids, key_weight, value_weight, out_grad):
    tok = latents.shape[0]
    heads = key_weight.shape[1] // NOPE
    steps = heads // PAIR
    line = n // 2
    rows = LATENT // n
    lag = max(Y_LAG + Z_LAG * (line - 1), F_LAG * (line - 1) + 4)
    grid_steps = steps + max(lag, 4)
    keys = (REACH + 1) * tok
    width = LATENT + ROPE
    ids = doc_ids.reshape(1, tok)
    wide = width + 64
    whole = pl.BlockSpec(memory_space=pltpu.VMEM)

    def at(lag_by):
        return lambda j: (0, jnp.clip(j - lag_by, 0, steps - 1))

    dma = pltpu.SemaphoreType.DMA
    att, lg, kwg, vwg = pl.pallas_call(
        functools.partial(kernel, n, hn, steps, grid_steps, lag),
        grid=(grid_steps,),
        out_shape=(
            pltpu.HBM((tok, heads * VDIM), BF16),
            pltpu.HBM((tok, width), F32),
            pltpu.HBM((rows, heads * NOPE), F32),
            pltpu.HBM((rows, heads * VDIM), F32),
        ),
        in_specs=[
            whole,
            whole,
            pl.BlockSpec((tok, PAIR * (NOPE + ROPE)), at(0)),
            pl.BlockSpec((tok, PAIR * VDIM), at(0)),
            pl.BlockSpec((LATENT, PAIR * NOPE), at(0)),
            pl.BlockSpec((LATENT, PAIR * VDIM), at(0)),
        ],
        out_specs=(
            pl.BlockSpec((tok, PAIR * VDIM), at(0)),
            whole,
            pl.BlockSpec((rows, PAIR * NOPE), at(lag)),
            pl.BlockSpec((rows, PAIR * VDIM), at(lag)),
        ),
        scratch_shapes=[
            pltpu.VMEM((hn, tok // hn, wide), BF16),
            pltpu.VMEM((REACH + 1, hn, tok // hn, wide), BF16),
            pltpu.VMEM((LATENT, keys), BF16),
            pltpu.VMEM((keys, tok), F32),
            pltpu.VMEM((keys, width), F32),
            pltpu.VMEM((steps, 2, line, rows, PAIR * (NOPE + VDIM)), BF16),
            pltpu.VMEM((steps, line, rows, PAIR * (NOPE + VDIM)), BF16),
            pltpu.VMEM((steps, 2, line, rows, PAIR * (NOPE + VDIM)), BF16),
            pltpu.VMEM((steps, 2, line, rows, PAIR * (NOPE + VDIM)), BF16),
            pltpu.VMEM((REACH, tok, width), BF16),
            pltpu.VMEM((REACH, tok, width), BF16),
            pltpu.VMEM((hn, tok, width), BF16),
            dma((REACH,)), dma((REACH,)),
            dma((max(hn - 1, 1), REACH)), dma((hn, REACH)),
            dma((steps,)), dma((steps,)),
            dma((steps, line)), dma((steps, line)), dma((steps, line)),
            dma((REACH,)), dma((REACH,)),
            dma((max(hn - 1, 1),)), dma((hn,)),
        ],
        compiler_params=pltpu.CompilerParams(
            collective_id=0,
            has_side_effects=True,
            dimension_semantics=("arbitrary",),
            vmem_limit_bytes=60 * 1024 * 1024,
        ),
    )(latents, ids, queries, out_grad, key_weight, value_weight)
    return att, lg, kwg, vwg


def solution(mesh):
    in_specs = (
        P("seq", "head"),
        P("seq", None),
        P("seq"),
        P(None, "head"),
        P(None, "head"),
        P("seq", "head"),
    )
    out_specs = (P("seq", "head"), P("seq", None), P("seq", "head"), P("seq", "head"))
    body = functools.partial(per_device, mesh.shape["seq"], mesh.shape["head"])
    return jax.shard_map(
        body, mesh=mesh, in_specs=in_specs, out_specs=out_specs, check_vma=False
    )
```
